32 devices in a mesh: ep: 32 (over z, y, x, core).
Axes of the slice: x: 2, y: 2, z: 4, core: 2. Of those that a mesh axis runs over, the one named last changes fastest.
Arguments:
- x_in: bfloat16 [12288, 2048], P('ep')
- route_idx: int32 [12288, 8], P('ep')
- gate_w: bfloat16 [12288, 8], P('ep')
- dy_in: bfloat16 [12288, 2048], P('ep')
- w_gate: bfloat16 [32, 2048, 1024], P('ep')
- w_up: bfloat16 [32, 2048, 1024], P('ep')
- w_down: bfloat16 [32, 1024, 2048], P('ep')
- hot_gate: bfloat16 [2048, 1024], replicated
- hot_up: bfloat16 [2048, 1024], replicated
- hot_down: bfloat16 [1024, 2048], replicated
Outputs:
- output 1: bfloat16 [12288, 2048], P('ep')
- output 2: bfloat16 [12288, 2048], P('ep')
- output 3: float32 [32, 2048, 1024], P('ep')
- output 4: float32 [32, 2048, 1024], P('ep')
- output 5: float32 [32, 1024, 2048], P('ep')
- output 6: float32 [2048, 1024], P(None, 'ep')
- output 7: float32 [2048, 1024], P(None, 'ep')
- output 8: float32 [1024, 2048], P('ep')
All inputs are finite; a program needn't handle non-finite values.
Results may differ from the reference program's by a relative error of at most 0.0107406.
Values are sent between devices in bfloat16 or wider.
A program may use at most 1 GiB of HBM per device.

```python
import jax
import jax.numpy as jnp
from jax import lax

N_DEV = 32
TOK_DEV = 384
D_MODEL = 2048
D_FF = 1024
TOP_K = 8

SLOT_CAP = min(TOK_DEV, 2 * TOK_DEV * TOP_K // N_DEV)
HOT_CAP = 3 * TOK_DEV // 4
TOTAL = N_DEV * TOK_DEV


def draw_routes(rng_key):
    heavy_key, weight_key, hot_key, pick_key, order_key, shift_key = jax.random.split(rng_key, 6)
    expert_ids = jnp.arange(N_DEV, dtype=jnp.int32)
    heavy = jax.random.randint(heavy_key, (N_DEV,), 0, N_DEV)
    is_heavy = expert_ids[None, :] == heavy[:, None]
    weight = jnp.where(is_heavy, 0, jax.random.randint(weight_key, (N_DEV, N_DEV), 1, 9))
    hot_count = jax.random.randint(hot_key, (N_DEV,), HOT_CAP // 4, HOT_CAP + 1)
    hot_count = jnp.where(expert_ids == jax.random.randint(pick_key, (), 0, N_DEV), HOT_CAP, hot_count)
    rest = TOK_DEV * TOP_K - hot_count - SLOT_CAP
    base = jnp.minimum((rest[:, None] * weight) // jnp.sum(weight, axis=1, keepdims=True), SLOT_CAP)
    room = jnp.where(is_heavy, 0, SLOT_CAP - base)
    deficit = rest - jnp.sum(base, axis=1)
    before = jnp.cumsum(room, axis=1) - room
    extra = jnp.minimum(jnp.maximum(deficit[:, None] - before, 0), room)
    load = base + extra + jnp.where(is_heavy, SLOT_CAP, 0)
    bounds = jnp.cumsum(jnp.concatenate([load, hot_count[:, None]], axis=1), axis=1)
    positions = jnp.arange(TOK_DEV * TOP_K, dtype=jnp.int32)
    ordered = jax.vmap(lambda bound_row: jnp.searchsorted(bound_row, positions, side='right'))(bounds)
    grid = ordered.reshape(N_DEV, TOP_K, TOK_DEV).transpose(0, 2, 1)
    token_order = jax.vmap(lambda sub_key: jax.random.permutation(sub_key, TOK_DEV))(jax.random.split(order_key, N_DEV))
    grid = jnp.take_along_axis(grid, token_order[:, :, None], axis=1)
    shift = jax.random.randint(shift_key, (N_DEV, TOK_DEV, 1), 0, TOP_K)
    col_index = (jnp.arange(TOP_K, dtype=jnp.int32)[None, None, :] + shift) % TOP_K
    grid = jnp.take_along_axis(grid, col_index, axis=2)
    return grid.reshape(TOTAL, TOP_K).astype(jnp.int32)


def setup_inputs(seed: int = 0) -> dict:
    sub_keys = jax.random.split(jax.random.key(seed), 10)
    in_scale = D_MODEL ** -0.5
    hid_scale = D_FF ** -0.5
    x_in = jax.random.normal(sub_keys[0], (TOTAL, D_MODEL), jnp.float32).astype(jnp.bfloat16)
    route_idx = draw_routes(sub_keys[1])
    gate_w = jax.random.uniform(sub_keys[2], (TOTAL, TOP_K), jnp.float32, 0.5, 1.5).astype(jnp.bfloat16)
    dy_in = jax.random.normal(sub_keys[3], (TOTAL, D_MODEL), jnp.float32).astype(jnp.bfloat16)
    w_gate = (jax.random.normal(sub_keys[4], (N_DEV, D_MODEL, D_FF), jnp.float32) * in_scale).astype(jnp.bfloat16)
    w_up = (jax.random.normal(sub_keys[5], (N_DEV, D_MODEL, D_FF), jnp.float32) * in_scale).astype(jnp.bfloat16)
    w_down = (jax.random.normal(sub_keys[6], (N_DEV, D_FF, D_MODEL), jnp.float32) * hid_scale).astype(jnp.bfloat16)
    hot_gate = (jax.random.normal(sub_keys[7], (D_MODEL, D_FF), jnp.float32) * in_scale).astype(jnp.bfloat16)
    hot_up = (jax.random.normal(sub_keys[8], (D_MODEL, D_FF), jnp.float32) * in_scale).astype(jnp.bfloat16)
    hot_down = (jax.random.normal(sub_keys[9], (D_FF, D_MODEL), jnp.float32) * hid_scale).astype(jnp.bfloat16)
    return {'x_in': x_in, 'route_idx': route_idx, 'gate_w': gate_w, 'dy_in': dy_in, 'w_gate': w_gate, 'w_up': w_up, 'w_down': w_down, 'hot_gate': hot_gate, 'hot_up': hot_up, 'hot_down': hot_down}


def silu_parts(pre_gate):
    sig_val = jax.nn.sigmoid(pre_gate)
    return pre_gate * sig_val, sig_val * (1.0 + pre_gate * (1.0 - sig_val))


def expert_pass(x_rows, d_rows, gate_mat, up_mat, down_mat):
    u_val = jnp.dot(x_rows, gate_mat, preferred_element_type=jnp.float32)
    v_val = jnp.dot(x_rows, up_mat, preferred_element_type=jnp.float32)
    silu_val, silu_grad = silu_parts(u_val)
    hidden = (silu_val * v_val).astype(jnp.bfloat16)
    result = jnp.dot(hidden, down_mat, preferred_element_type=jnp.float32).astype(jnp.bfloat16)
    grad_hidden = jnp.dot(d_rows, down_mat.T, preferred_element_type=jnp.float32).astype(jnp.bfloat16).astype(jnp.float32)
    grad_u = (grad_hidden * v_val * silu_grad).astype(jnp.bfloat16)
    grad_v = (grad_hidden * silu_val).astype(jnp.bfloat16)
    grad_x = (jnp.dot(grad_u, gate_mat.T, preferred_element_type=jnp.float32) + jnp.dot(grad_v, up_mat.T, preferred_element_type=jnp.float32)).astype(jnp.bfloat16)
    grad_gate = jnp.dot(x_rows.T, grad_u, preferred_element_type=jnp.float32)
    grad_up = jnp.dot(x_rows.T, grad_v, preferred_element_type=jnp.float32)
    grad_down = jnp.dot(hidden.T, d_rows, preferred_element_type=jnp.float32)
    return result, grad_x, (grad_gate, grad_up, grad_down)


def reference(x_in, route_idx, gate_w, dy_in, w_gate, w_up, w_down, hot_gate, hot_up, hot_down):
    flat_ids = route_idx.reshape(-1)
    n_assign = flat_ids.shape[0]
    order = jnp.argsort(flat_ids, stable=True)
    starts = jnp.searchsorted(flat_ids[order], jnp.arange(N_DEV + 2, dtype=jnp.int32), side='left')
    gate_flat = gate_w.reshape(-1)

    def take_block(first, last, max_rows):
        position = first + jnp.arange(max_rows, dtype=jnp.int32)
        assign = jnp.where(position < last, order[jnp.minimum(position, n_assign - 1)], n_assign)
        token = assign // TOP_K
        x_rows = jnp.take(x_in, token, axis=0, mode='fill', fill_value=0)
        gate_rows = jnp.take(gate_flat, assign, mode='fill', fill_value=0).astype(jnp.float32)
        dy_rows = jnp.take(dy_in, token, axis=0, mode='fill', fill_value=0).astype(jnp.float32)
        d_rows = (gate_rows[:, None] * dy_rows).astype(jnp.bfloat16)
        return token, gate_rows, x_rows, d_rows

    def add_block(sums, token, gate_rows, result, grad_x):
        y_sum, dx_sum = sums
        y_sum = y_sum.at[token].add(gate_rows[:, None] * result.astype(jnp.float32), mode='drop')
        dx_sum = dx_sum.at[token].add(grad_x.astype(jnp.float32), mode='drop')
        return y_sum, dx_sum

    def regular_step(sums, expert_args):
        gate_mat, up_mat, down_mat, first, last = expert_args
        token, gate_rows, x_rows, d_rows = take_block(first, last, N_DEV * SLOT_CAP)
        result, grad_x, grads = expert_pass(x_rows, d_rows, gate_mat, up_mat, down_mat)
        return add_block(sums, token, gate_rows, result, grad_x), grads

    zero_sum = jnp.zeros((TOTAL, D_MODEL), jnp.float32)
    sums, (dw_gate, dw_up, dw_down) = lax.scan(regular_step, (zero_sum, zero_sum), (w_gate, w_up, w_down, starts[:N_DEV], starts[1:N_DEV + 1]))
    token, gate_rows, x_rows, d_rows = take_block(starts[N_DEV], starts[N_DEV + 1], N_DEV * HOT_CAP)
    result, grad_x, (dhot_gate, dhot_up, dhot_down) = expert_pass(x_rows, d_rows, hot_gate, hot_up, hot_down)
    y_sum, dx_sum = add_block(sums, token, gate_rows, result, grad_x)
    return (y_sum.astype(jnp.bfloat16), dx_sum.astype(jnp.bfloat16), dw_gate, dw_up, dw_down, dhot_gate, dhot_up, dhot_down)
```

```python
import functools

import jax
import jax.numpy as jnp
from jax import lax
from jax.experimental import pallas as pl
from jax.experimental.pallas import tpu as pltpu
from jax.sharding import PartitionSpec as P

BF16 = jnp.bfloat16
F32 = jnp.float32
CONTRACT_LAST = (((1,), (1,)), ((), ()))
CONTRACT_FIRST = (((0,), (0,)), ((), ()))


def dot(a, b, dims=(((1,), (0,)), ((), ()))):
    return lax.dot_general(a, b, dims, preferred_element_type=F32)


def silu_parts(pre_gate):
    sig_val = jax.nn.sigmoid(pre_gate)
    return pre_gate * sig_val, sig_val * (1.0 + pre_gate * (1.0 - sig_val))


def hot_grad_kernel(x_ref, dy_ref, gate_ref, mask_ref, wgu_ref, wd_ref, dgu_ref, dd_ref):
    half = wd_ref.shape[0]

    @pl.when(pl.program_id(0) == 0)
    def _():
        dgu_ref[...] = jnp.zeros_like(dgu_ref)
        dd_ref[...] = jnp.zeros_like(dd_ref)

    x_rows = x_ref[...]
    q_rows = (gate_ref[...] * dy_ref[...].astype(F32)).astype(BF16)
    chosen = mask_ref[...] > 0.0
    uv = dot(x_rows, wgu_ref[...])
    p_val = dot(q_rows, wd_ref[...], CONTRACT_LAST).astype(BF16).astype(F32)
    u_val, v_val = uv[:, :half], uv[:, half:]
    silu_val, silu_grad = silu_parts(u_val)
    hidden = jnp.where(chosen, silu_val * v_val, 0.0).astype(BF16)
    du = jnp.where(chosen, p_val * v_val * silu_grad, 0.0).astype(BF16)
    dv = jnp.where(chosen, p_val * silu_val, 0.0).astype(BF16)
    dgu_ref[...] += dot(jnp.concatenate([du, dv], axis=1), x_rows, CONTRACT_FIRST)
    dd_ref[...] += dot(hidden, q_rows, CONTRACT_FIRST)


def hot_grads(x_all, dy_all, gate_col, mask_col, wgu, wd, block=512):
    total, d_model = x_all.shape
    half = wd.shape[0]
    flops = 2 * total * d_model * (6 * half)
    return pl.pallas_call(
        hot_grad_kernel,
        grid=(total // block,),
        in_specs=[
            pl.BlockSpec((block, d_model), lambda i: (i, 0)),
            pl.BlockSpec((block, d_model), lambda i: (i, 0)),
            pl.BlockSpec((block, 1), lambda i: (i, 0)),
            pl.BlockSpec((block, 1), lambda i: (i, 0)),
            pl.BlockSpec((d_model, 2 * half), lambda i: (0, 0)),
            pl.BlockSpec((half, d_model), lambda i: (0, 0)),
        ],
        out_specs=[
            pl.BlockSpec((2 * half, d_model), lambda i: (0, 0)),
            pl.BlockSpec((half, d_model), lambda i: (0, 0)),
        ],
        out_shape=[jax.ShapeDtypeStruct((2 * half, d_model), F32), jax.ShapeDtypeStruct((half, d_model), F32)],
        cost_estimate=pl.CostEstimate(flops=flops, bytes_accessed=4 * total * d_model, transcendentals=0),
        compiler_params=pltpu.CompilerParams(dimension_semantics=("arbitrary",), vmem_limit_bytes=50 * 2**20),
        name="hot_grads",
    )(x_all, dy_all, gate_col, mask_col, wgu, wd)


def solution(mesh):
    n_dev = mesh.shape['ep']

    def local_step(x_loc, route_loc, gate_loc, dy_loc, w_gate, w_up, w_down, hot_gate, hot_up, hot_down):
        tok, top_k = route_loc.shape
        d_model = x_loc.shape[1]
        d_ff = w_gate.shape[2]
        total = n_dev * tok
        slot_cap = min(tok, 2 * tok * top_k // n_dev)
        n_rows = n_dev * slot_cap
        sub = d_model // 128
        me = lax.axis_index('ep')

        meta = jnp.concatenate([route_loc.T.astype(F32), gate_loc.T.astype(F32)], axis=0)
        meta_all = lax.all_gather(meta, 'ep')
        x_all = lax.all_gather(x_loc, 'ep', tiled=True)
        dy_all = lax.all_gather(dy_loc, 'ep', tiled=True)
        route_all, gate_all = meta_all[:, :top_k], meta_all[:, top_k:]

        mine = route_all == me.astype(F32)
        has = jnp.any(mine, axis=1)
        gate_mine = jnp.sum(jnp.where(mine, gate_all, 0.0), axis=1)
        cnt = jnp.sum(has.astype(jnp.int32), axis=1)
        ends = jnp.cumsum(cnt)
        starts = ends - cnt
        tri = (jnp.arange(tok)[:, None] <= jnp.arange(tok)[None, :]).astype(BF16)
        incl = dot(has.astype(BF16), tri)
        slot = jnp.where(has, incl, 0.0)
        row_ids = jnp.arange(n_rows, dtype=jnp.int32)
        ours = (row_ids[:, None] >= starts[None, :]) & (row_ids[:, None] < ends[None, :])
        source = jnp.sum(jnp.where(ours, jnp.arange(n_dev)[None, :], 0), axis=1)
        local = row_ids + 1 - jnp.sum(jnp.where(ours, starts[None, :], 0), axis=1)
        pick = ours.astype(BF16)
        match = dot(pick, slot.astype(BF16)) == local[:, None].astype(F32)
        token = source * tok + jnp.sum(jnp.where(match, jnp.arange(tok)[None, :], 0), axis=1)
        gate_row = jnp.sum(jnp.where(match, dot(pick, gate_mine.astype(BF16)), 0.0), axis=1)
        valid = (row_ids < ends[-1])[:, None]

        hot_all = route_all == float(n_dev)
        hot_mask = jnp.any(hot_all, axis=1).astype(F32).reshape(total, 1)
        hot_gate_w = jnp.sum(jnp.where(hot_all, gate_all, 0.0), axis=1).reshape(total, 1)
        own_hot = route_loc == n_dev
        own_hot_mask = jnp.any(own_hot, axis=1)[:, None]
        own_hot_gate = jnp.sum(jnp.where(own_hot, gate_loc.astype(F32), 0.0), axis=1)[:, None]

        place = jnp.clip(incl.astype(jnp.int32) + starts[:, None] - 1, 0, n_rows - 1).reshape(total)
        has_col = has.reshape(total, 1)
        gate_col = gate_mine.reshape(total, 1)

        def sum_choices(rows, weight, has_col):
            spread = rows.at[place].get(mode='promise_in_bounds').astype(F32)
            return lax.psum_scatter(jnp.where(has_col, spread * weight, 0.0), 'ep', scatter_dimension=0, tiled=True)

        wg, wu, wd = w_gate[0], w_up[0], w_down[0]
        x_rows = jnp.take(x_all, token, axis=0, mode='clip')
        u_val = dot(x_rows, wg)
        v_val = dot(x_rows, wu)
        silu_val, silu_grad = silu_parts(u_val)
        hidden = jnp.where(valid, silu_val * v_val, 0.0).astype(BF16)
        y_reg = sum_choices(dot(hidden, wd).astype(BF16), gate_col, has_col)

        q_rows = (gate_row[:, None] * jnp.take(dy_all, token, axis=0, mode='clip').astype(F32)).astype(BF16)
        p_val = dot(q_rows, wd, CONTRACT_LAST).astype(BF16).astype(F32)
        du = jnp.where(valid, p_val * v_val * silu_grad, 0.0).astype(BF16)
        dv = jnp.where(valid, p_val * silu_val, 0.0).astype(BF16)
        dx_reg = sum_choices((dot(du, wg, CONTRACT_LAST) + dot(dv, wu, CONTRACT_LAST)).astype(BF16), 1.0, lax.optimization_barrier(has_col))
        grad_gate = dot(x_rows, du, CONTRACT_FIRST)
        grad_up = dot(x_rows, dv, CONTRACT_FIRST)
        grad_down = dot(hidden, q_rows, CONTRACT_FIRST)

        hu = dot(x_loc, hot_gate)
        hv = dot(x_loc, hot_up)
        h_silu, h_silu_grad = silu_parts(hu)
        h_hidden = (h_silu * hv).astype(BF16)
        h_out = dot(h_hidden, hot_down).astype(BF16)
        h_q = (own_hot_gate * dy_loc.astype(F32)).astype(BF16)
        h_p = dot(h_q, hot_down, CONTRACT_LAST).astype(BF16).astype(F32)
        h_du = jnp.where(own_hot_mask, h_p * hv * h_silu_grad, 0.0).astype(BF16)
        h_dv = jnp.where(own_hot_mask, h_p * h_silu, 0.0).astype(BF16)
        h_r = (dot(h_du, hot_gate, CONTRACT_LAST) + dot(h_dv, hot_up, CONTRACT_LAST)).astype(BF16)
        y_hot = jnp.where(own_hot_mask, own_hot_gate * h_out.astype(F32), 0.0)

        part = d_ff // n_dev
        pad = ((0, 0), (0, 128 - part))
        g_part = jnp.pad(lax.dynamic_slice_in_dim(hot_gate, me * part, part, 1), pad)
        u_part = jnp.pad(lax.dynamic_slice_in_dim(hot_up, me * part, part, 1), pad)
        d_part = jnp.pad(lax.dynamic_slice_in_dim(hot_down, me * part, part, 0), ((0, 128 - part), (0, 0)))
        dgu, dd = hot_grads(x_all, dy_all, hot_gate_w, hot_mask, jnp.concatenate([g_part, u_part], axis=1), d_part)
        hot_dgate = dgu[:part].T
        hot_dup = dgu[128:128 + part].T
        hot_ddown = dd[:part]

        y_loc = y_reg + y_hot
        dx_loc = dx_reg + h_r.astype(F32)
        return (y_loc.astype(BF16), dx_loc.astype(BF16), grad_gate[None], grad_up[None], grad_down[None],
                hot_dgate, hot_dup, hot_ddown)

    row_spec = P('ep', None)
    expert_spec = P('ep', None, None)
    whole_spec = P(None, None)
    return jax.shard_map(local_step, mesh=mesh, in_specs=(row_spec, row_spec, row_spec, row_spec, expert_spec, expert_spec, expert_spec, whole_spec, whole_spec, whole_spec), out_specs=(row_spec, row_spec, expert_spec, expert_spec, expert_spec, P(None, 'ep'), P(None, 'ep'), P('ep', None)), check_vma=False)
```

```python
import jax
import jax.numpy as jnp
from jax import lax
from jax.experimental import pallas as pl
from jax.experimental.pallas import tpu as pltpu
from jax.sharding import PartitionSpec as P


BF16 = jnp.bfloat16
F32 = jnp.float32
CONTRACT_LAST = (((1,), (1,)), ((), ()))
CONTRACT_FIRST = (((0,), (0,)), ((), ()))


def dot(a, b, dims=(((1,), (0,)), ((), ()))):
    return lax.dot_general(a, b, dims, preferred_element_type=F32)


def silu_parts(pre_gate):
    sig_val = jax.nn.sigmoid(pre_gate)
    return pre_gate * sig_val, sig_val * (1.0 + pre_gate * (1.0 - sig_val))


def hot_grad_kernel(x_ref, dy_ref, gate_ref, mask_ref, wgu_ref, wd_ref, dgu_ref, dd_ref):
    half = wd_ref.shape[0]

    @pl.when(pl.program_id(0) == 0)
    def _():
        dgu_ref[...] = jnp.zeros_like(dgu_ref)
        dd_ref[...] = jnp.zeros_like(dd_ref)

    x_rows = x_ref[...]
    q_rows = (gate_ref[...] * dy_ref[...].astype(F32)).astype(BF16)
    chosen = mask_ref[...] > 0.0
    uv = dot(x_rows, wgu_ref[...])
    p_val = dot(q_rows, wd_ref[...], CONTRACT_LAST).astype(BF16).astype(F32)
    u_val, v_val = uv[:, :half], uv[:, half:]
    silu_val, silu_grad = silu_parts(u_val)
    hidden = jnp.where(chosen, silu_val * v_val, 0.0).astype(BF16)
    du = jnp.where(chosen, p_val * v_val * silu_grad, 0.0).astype(BF16)
    dv = jnp.where(chosen, p_val * silu_val, 0.0).astype(BF16)
    dgu_ref[...] += dot(jnp.concatenate([du, dv], axis=1), x_rows, CONTRACT_FIRST)
    dd_ref[...] += dot(hidden, q_rows, CONTRACT_FIRST)


def hot_grads(x_all, dy_all, gate_col, mask_col, wgu, wd, block=512):
    total, d_model = x_all.shape
    half = wd.shape[0]
    flops = 2 * total * d_model * (6 * half)
    return pl.pallas_call(
        hot_grad_kernel,
        grid=(total // block,),
        in_specs=[
            pl.BlockSpec((block, d_model), lambda i: (i, 0)),
            pl.BlockSpec((block, d_model), lambda i: (i, 0)),
            pl.BlockSpec((block, 1), lambda i: (i, 0)),
            pl.BlockSpec((block, 1), lambda i: (i, 0)),
            pl.BlockSpec((d_model, 2 * half), lambda i: (0, 0)),
            pl.BlockSpec((half, d_model), lambda i: (0, 0)),
        ],
        out_specs=[
            pl.BlockSpec((2 * half, d_model), lambda i: (0, 0)),
            pl.BlockSpec((half, d_model), lambda i: (0, 0)),
        ],
        out_shape=[jax.ShapeDtypeStruct((2 * half, d_model), F32), jax.ShapeDtypeStruct((half, d_model), F32)],
        cost_estimate=pl.CostEstimate(flops=flops, bytes_accessed=4 * total * d_model, transcendentals=0),
        compiler_params=pltpu.CompilerParams(dimension_semantics=("arbitrary",), vmem_limit_bytes=50 * 2**20),
        name="hot_grads",
    )(x_all, dy_all, gate_col, mask_col, wgu, wd)


def solution(mesh):
    n_dev = mesh.shape['ep']

    def local_step(x_loc, route_loc, gate_loc, dy_loc, w_gate, w_up, w_down, hot_gate, hot_up, hot_down):
        tok, top_k = route_loc.shape
        d_model = x_loc.shape[1]
        d_ff = w_gate.shape[2]
        total = n_dev * tok
        slot_cap = min(tok, 2 * tok * top_k // n_dev)
        n_rows = n_dev * slot_cap
        me = lax.axis_index('ep')

        meta = jnp.concatenate([route_loc.T.astype(F32), gate_loc.T.astype(F32)], axis=0)
        meta_all = lax.all_gather(meta, 'ep')
        x_all = lax.all_gather(x_loc, 'ep', tiled=True)
        dy_all = lax.all_gather(dy_loc, 'ep', tiled=True)
        route_all, gate_all = meta_all[:, :top_k], meta_all[:, top_k:]

        mine = route_all == me.astype(F32)
        has = jnp.any(mine, axis=1)
        gate_mine = jnp.sum(jnp.where(mine, gate_all, 0.0), axis=1)
        tri = (jnp.arange(tok)[:, None] <= jnp.arange(tok)[None, :]).astype(BF16)
        order = jnp.where(has, dot(has.astype(BF16), tri), 0.0)[:, None, :]
        match = order == jnp.arange(1, slot_cap + 1).astype(F32)[None, :, None]

        def pick_rows(picker, rows):
            picked = lax.dot_general(picker.astype(BF16), rows.reshape(n_dev, tok, d_model), (((2,), (1,)), ((0,), (0,))), preferred_element_type=F32)
            return picked.astype(BF16).reshape(n_rows, d_model)

        hot_all = route_all == float(n_dev)
        hot_mask = jnp.any(hot_all, axis=1).astype(F32).reshape(total, 1)
        hot_gate_w = jnp.sum(jnp.where(hot_all, gate_all, 0.0), axis=1).reshape(total, 1)
        own_hot = route_loc == n_dev
        own_hot_mask = jnp.any(own_hot, axis=1)[:, None]
        own_hot_gate = jnp.sum(jnp.where(own_hot, gate_loc.astype(F32), 0.0), axis=1)[:, None]

        one_hot = route_loc[:, :, None] == jnp.arange(n_dev, dtype=jnp.int32)[None, None, :]
        own_has = jnp.any(one_hot, axis=1)
        own_gate = jnp.sum(jnp.where(one_hot, gate_loc.astype(F32)[:, :, None], 0.0), axis=1)
        rank = jnp.where(own_has, dot(tri, own_has.astype(BF16), CONTRACT_FIRST) - 1.0, -1.0)
        col = jnp.arange(n_rows, dtype=jnp.int32)
        widen = (jnp.arange(n_dev)[:, None] == col[None, :] // slot_cap).astype(BF16)
        back_match = dot(rank.astype(BF16), widen) == (col % slot_cap).astype(F32)[None, :]
        back_ones = back_match.astype(BF16)
        back_gates = jnp.where(back_match, dot(own_gate.astype(BF16), widen), 0.0).astype(BF16)

        def give_back(rows):
            return lax.all_to_all(rows.astype(BF16), 'ep', 0, 0, tiled=True)

        wg, wu, wd = w_gate[0], w_up[0], w_down[0]
        x_rows = pick_rows(match, x_all)
        u_val = dot(x_rows, wg)
        v_val = dot(x_rows, wu)
        hidden = (silu_parts(u_val)[0] * v_val).astype(BF16)
        hidden, u_val, v_val = lax.optimization_barrier((hidden, u_val, v_val))
        o_rows = dot(hidden, wd).astype(BF16)
        back_o = give_back(o_rows)
        gate_late, _ = lax.optimization_barrier((gate_mine, o_rows))

        q_rows = pick_rows(jnp.where(match, gate_late[:, None, :], 0.0), dy_all)
        p_val = dot(q_rows, wd, CONTRACT_LAST).astype(BF16).astype(F32)
        silu_val, silu_grad = silu_parts(u_val)
        du = (p_val * v_val * silu_grad).astype(BF16)
        dv = (p_val * silu_val).astype(BF16)
        r_rows = (dot(du, wg, CONTRACT_LAST) + dot(dv, wu, CONTRACT_LAST)).astype(BF16)
        r_rows, back_o = lax.optimization_barrier((r_rows, back_o))
        back_r = give_back(r_rows)
        grad_gate = dot(x_rows, du, CONTRACT_FIRST)
        grad_up = dot(x_rows, dv, CONTRACT_FIRST)
        grad_down = dot(hidden, q_rows, CONTRACT_FIRST)

        hu = dot(x_loc, hot_gate)
        hv = dot(x_loc, hot_up)
        h_silu, h_silu_grad = silu_parts(hu)
        h_hidden = (h_silu * hv).astype(BF16)
        h_out = dot(h_hidden, hot_down).astype(BF16)
        h_q = (own_hot_gate * dy_loc.astype(F32)).astype(BF16)
        h_p = dot(h_q, hot_down, CONTRACT_LAST).astype(BF16).astype(F32)
        h_du = jnp.where(own_hot_mask, h_p * hv * h_silu_grad, 0.0).astype(BF16)
        h_dv = jnp.where(own_hot_mask, h_p * h_silu, 0.0).astype(BF16)
        h_r = (dot(h_du, hot_gate, CONTRACT_LAST) + dot(h_dv, hot_up, CONTRACT_LAST)).astype(BF16)
        y_hot = jnp.where(own_hot_mask, own_hot_gate * h_out.astype(F32), 0.0)

        part = d_ff // n_dev
        pad = ((0, 0), (0, 128 - part))
        g_part = jnp.pad(lax.dynamic_slice_in_dim(hot_gate, me * part, part, 1), pad)
        u_part = jnp.pad(lax.dynamic_slice_in_dim(hot_up, me * part, part, 1), pad)
        d_part = jnp.pad(lax.dynamic_slice_in_dim(hot_down, me * part, part, 0), ((0, 128 - part), (0, 0)))
        dgu, dd = hot_grads(x_all, dy_all, hot_gate_w, hot_mask, jnp.concatenate([g_part, u_part], axis=1), d_part)
        hot_dgate = dgu[:part].T
        hot_dup = dgu[128:128 + part].T
        hot_ddown = dd[:part]

        y_loc = dot(back_gates, back_o) + y_hot
        dx_loc = dot(back_ones, back_r) + h_r.astype(F32)
        return (y_loc.astype(BF16), dx_loc.astype(BF16), grad_gate[None], grad_up[None], grad_down[None],
                hot_dgate, hot_dup, hot_ddown)

    row_spec = P('ep', None)
    expert_spec = P('ep', None, None)
    whole_spec = P(None, None)
    return jax.shard_map(local_step, mesh=mesh, in_specs=(row_spec, row_spec, row_spec, row_spec, expert_spec, expert_spec, expert_spec, whole_spec, whole_spec, whole_spec), out_specs=(row_spec, row_spec, expert_spec, expert_spec, expert_spec, P(None, 'ep'), P(None, 'ep'), P('ep', None)), check_vma=False)
```

```python
import jax
import jax.numpy as jnp
from jax import lax
from jax.experimental import pallas as pl
from jax.experimental.pallas import tpu as pltpu
from jax.sharding import PartitionSpec as P


BF16 = jnp.bfloat16
F32 = jnp.float32
CONTRACT_LAST = (((1,), (1,)), ((), ()))
CONTRACT_FIRST = (((0,), (0,)), ((), ()))


def dot(a, b, dims=(((1,), (0,)), ((), ()))):
    return lax.dot_general(a, b, dims, preferred_element_type=F32)


def silu_parts(pre_gate):
    sig_val = jax.nn.sigmoid(pre_gate)
    return pre_gate * sig_val, sig_val * (1.0 + pre_gate * (1.0 - sig_val))


def hot_grad_kernel(x_ref, dy_ref, gate_ref, mask_ref, wgu_ref, wd_ref, dgu_ref, dd_ref):
    half = wd_ref.shape[0]

    @pl.when(pl.program_id(0) == 0)
    def _():
        dgu_ref[...] = jnp.zeros_like(dgu_ref)
        dd_ref[...] = jnp.zeros_like(dd_ref)

    x_rows = x_ref[...]
    q_rows = (gate_ref[...] * dy_ref[...].astype(F32)).astype(BF16)
    chosen = mask_ref[...] > 0.0
    uv = dot(x_rows, wgu_ref[...])
    p_val = dot(q_rows, wd_ref[...], CONTRACT_LAST).astype(BF16).astype(F32)
    u_val, v_val = uv[:, :half], uv[:, half:]
    silu_val, silu_grad = silu_parts(u_val)
    hidden = jnp.where(chosen, silu_val * v_val, 0.0).astype(BF16)
    du = jnp.where(chosen, p_val * v_val * silu_grad, 0.0).astype(BF16)
    dv = jnp.where(chosen, p_val * silu_val, 0.0).astype(BF16)
    dgu_ref[...] += dot(jnp.concatenate([du, dv], axis=1), x_rows, CONTRACT_FIRST)
    dd_ref[...] += dot(hidden, q_rows, CONTRACT_FIRST)


def hot_grads(x_all, dy_all, gate_col, mask_col, wgu, wd, block=512):
    total, d_model = x_all.shape
    half = wd.shape[0]
    flops = 2 * total * d_model * (6 * half)
    return pl.pallas_call(
        hot_grad_kernel,
        grid=(total // block,),
        in_specs=[
            pl.BlockSpec((block, d_model), lambda i: (i, 0)),
            pl.BlockSpec((block, d_model), lambda i: (i, 0)),
            pl.BlockSpec((block, 1), lambda i: (i, 0)),
            pl.BlockSpec((block, 1), lambda i: (i, 0)),
            pl.BlockSpec((d_model, 2 * half), lambda i: (0, 0)),
            pl.BlockSpec((half, d_model), lambda i: (0, 0)),
        ],
        out_specs=[
            pl.BlockSpec((2 * half, d_model), lambda i: (0, 0)),
            pl.BlockSpec((half, d_model), lambda i: (0, 0)),
        ],
        out_shape=[jax.ShapeDtypeStruct((2 * half, d_model), F32), jax.ShapeDtypeStruct((half, d_model), F32)],
        cost_estimate=pl.CostEstimate(flops=flops, bytes_accessed=4 * total * d_model, transcendentals=0),
        compiler_params=pltpu.CompilerParams(dimension_semantics=("arbitrary",), vmem_limit_bytes=50 * 2**20),
        name="hot_grads",
    )(x_all, dy_all, gate_col, mask_col, wgu, wd)


def solution(mesh):
    n_dev = mesh.shape['ep']
    n_z = 4
    shifts = (2, 1, 3, 0)

    def local_step(x_loc, route_loc, gate_loc, dy_loc, w_gate, w_up, w_down, hot_gate, hot_up, hot_down):
        tok, top_k = route_loc.shape
        d_model = x_loc.shape[1]
        d_ff = w_gate.shape[2]
        total = n_dev * tok
        slot_cap = min(tok, 2 * tok * top_k // n_dev)
        n_rows = n_dev * slot_cap
        me = lax.axis_index('ep')

        meta = jnp.concatenate([route_loc.T.astype(F32), gate_loc.T.astype(F32)], axis=0)
        meta_all = lax.all_gather(meta, 'ep')
        x_all = lax.all_gather(x_loc, 'ep', tiled=True)
        dy_all = lax.all_gather(dy_loc, 'ep', tiled=True)
        route_all, gate_all = meta_all[:, :top_k], meta_all[:, top_k:]

        mine = route_all == me.astype(F32)
        has = jnp.any(mine, axis=1)
        gate_mine = jnp.sum(jnp.where(mine, gate_all, 0.0), axis=1)
        tri = (jnp.arange(tok)[:, None] <= jnp.arange(tok)[None, :]).astype(BF16)
        order = jnp.where(has, dot(has.astype(BF16), tri), 0.0)[:, None, :]
        match = order == jnp.arange(1, slot_cap + 1).astype(F32)[None, :, None]

        def pick_rows(picker, rows):
            picked = lax.dot_general(picker.astype(BF16), rows.reshape(n_dev, tok, d_model), (((2,), (1,)), ((0,), (0,))), preferred_element_type=F32)
            return picked.astype(BF16).reshape(n_rows, d_model)

        hot_all = route_all == float(n_dev)
        hot_mask = jnp.any(hot_all, axis=1).astype(F32).reshape(total, 1)
        hot_gate_w = jnp.sum(jnp.where(hot_all, gate_all, 0.0), axis=1).reshape(total, 1)
        own_hot = route_loc == n_dev
        own_hot_mask = jnp.any(own_hot, axis=1)[:, None]
        own_hot_gate = jnp.sum(jnp.where(own_hot, gate_loc.astype(F32), 0.0), axis=1)[:, None]

        plane = n_dev // n_z
        my_z, my_p = me // plane, me % plane
        groups = [[g * plane + i for i in range(plane)] for g in range(n_z)]
        col = jnp.arange(plane * slot_cap, dtype=jnp.int32)
        widen = (jnp.arange(plane)[:, None] == col[None, :] // slot_cap).astype(BF16)
        plane_ids = (my_z * plane + jnp.arange(plane)).astype(F32)

        def pickers(k):
            other = lax.dynamic_index_in_dim(meta_all, lax.rem(my_z + k, n_z) * plane + my_p, 0, keepdims=False)
            one_hot = other[:top_k, :, None] == plane_ids[None, None, :]
            chosen = jnp.any(one_hot, axis=0)
            weight = jnp.sum(jnp.where(one_hot, other[top_k:, :, None], 0.0), axis=0)
            rank = jnp.where(chosen, dot(tri, chosen.astype(BF16), CONTRACT_FIRST) - 1.0, -1.0)
            hit = dot(rank.astype(BF16), widen) == (col % slot_cap).astype(F32)[None, :]
            return jnp.where(hit, dot(weight.astype(BF16), widen), 0.0).astype(BF16), hit.astype(BF16)

        picks = {k: pickers(k) for k in shifts}

        def go_home(rows, which, before):
            rows = rows.reshape(n_z, plane * slot_cap, d_model)
            sums = []
            for k in shifts:
                part = lax.dynamic_index_in_dim(rows, lax.rem(my_z + k, n_z), 0, keepdims=False)
                if before is not None:
                    part, before = lax.optimization_barrier((part, before))
                before = lax.all_to_all(part, 'ep', 0, 0, axis_index_groups=groups, tiled=True)
                sums.append(dot(picks[k][which], before))
                if k:
                    sums[-1] = lax.ppermute(sums[-1], 'ep', [(d, (d + k * plane) % n_dev) for d in range(n_dev)])
            return sums[0] + sums[1] + sums[2] + sums[3], before

        wg, wu, wd = w_gate[0], w_up[0], w_down[0]
        x_rows = pick_rows(match, x_all)
        u_val = dot(x_rows, wg)
        v_val = dot(x_rows, wu)
        hidden = (silu_parts(u_val)[0] * v_val).astype(BF16)
        hidden, u_val, v_val = lax.optimization_barrier((hidden, u_val, v_val))
        o_rows = dot(hidden, wd).astype(BF16)
        y_reg, o_last = go_home(o_rows, 0, None)
        gate_late, _ = lax.optimization_barrier((gate_mine, o_rows))

        q_rows = pick_rows(jnp.where(match, gate_late[:, None, :], 0.0), dy_all)
        p_val = dot(q_rows, wd, CONTRACT_LAST).astype(BF16).astype(F32)
        silu_val, silu_grad = silu_parts(u_val)
        du = (p_val * v_val * silu_grad).astype(BF16)
        dv = (p_val * silu_val).astype(BF16)
        r_rows = (dot(du, wg, CONTRACT_LAST) + dot(dv, wu, CONTRACT_LAST)).astype(BF16)
        dx_reg, _ = go_home(r_rows, 1, o_last)
        grad_gate = dot(x_rows, du, CONTRACT_FIRST)
        grad_up = dot(x_rows, dv, CONTRACT_FIRST)
        grad_down = dot(hidden, q_rows, CONTRACT_FIRST)

        hu = dot(x_loc, hot_gate)
        hv = dot(x_loc, hot_up)
        h_silu, h_silu_grad = silu_parts(hu)
        h_hidden = (h_silu * hv).astype(BF16)
        h_out = dot(h_hidden, hot_down).astype(BF16)
        h_q = (own_hot_gate * dy_loc.astype(F32)).astype(BF16)
        h_p = dot(h_q, hot_down, CONTRACT_LAST).astype(BF16).astype(F32)
        h_du = jnp.where(own_hot_mask, h_p * hv * h_silu_grad, 0.0).astype(BF16)
        h_dv = jnp.where(own_hot_mask, h_p * h_silu, 0.0).astype(BF16)
        h_r = (dot(h_du, hot_gate, CONTRACT_LAST) + dot(h_dv, hot_up, CONTRACT_LAST)).astype(BF16)
        y_hot = jnp.where(own_hot_mask, own_hot_gate * h_out.astype(F32), 0.0)

        part = d_ff // n_dev
        pad = ((0, 0), (0, 128 - part))
        g_part = jnp.pad(lax.dynamic_slice_in_dim(hot_gate, me * part, part, 1), pad)
        u_part = jnp.pad(lax.dynamic_slice_in_dim(hot_up, me * part, part, 1), pad)
        d_part = jnp.pad(lax.dynamic_slice_in_dim(hot_down, me * part, part, 0), ((0, 128 - part), (0, 0)))
        dgu, dd = hot_grads(x_all, dy_all, hot_gate_w, hot_mask, jnp.concatenate([g_part, u_part], axis=1), d_part)
        hot_dgate = dgu[:part].T
        hot_dup = dgu[128:128 + part].T
        hot_ddown = dd[:part]

        y_loc = y_reg + y_hot
        dx_loc = dx_reg + h_r.astype(F32)
        return (y_loc.astype(BF16), dx_loc.astype(BF16), grad_gate[None], grad_up[None], grad_down[None],
                hot_dgate, hot_dup, hot_ddown)

    row_spec = P('ep', None)
    expert_spec = P('ep', None, None)
    whole_spec = P(None, None)
    return jax.shard_map(local_step, mesh=mesh, in_specs=(row_spec, row_spec, row_spec, row_spec, expert_spec, expert_spec, expert_spec, whole_spec, whole_spec, whole_spec), out_specs=(row_spec, row_spec, expert_spec, expert_spec, expert_spec, P(None, 'ep'), P(None, 'ep'), P('ep', None)), check_vma=False)
```
